32 devices in a mesh: groups: 2 (over x), docs: 16 (over z, y, core).
Axes of the slice: x: 2, y: 2, z: 4, core: 2. Of those that a mesh axis runs over, the one named last changes fastest.
Arguments:
- sentences: bfloat16 [65536, 1280], P(('groups', 'docs')), parts along dimension 0, may hold values from -10 to 10
- sent_doc: int32 [65536], P('groups'), parts along dimension 0, may hold values from 0 to 2047, never falling along the last dimension, each value on 1 to 32 neighbouring positions
- images: bfloat16 [8192, 1280], P(('groups', 'docs')), parts along dimension 0, may hold values from -30 to 30
- image_owner: int32 [8192, 1], P(('groups', 'docs')), parts along dimension 0, may hold values from 0 to 15, as said below
- anchor: int32 [8192], P(('groups', 'docs')), parts along dimension 0, may hold values from 0 to 2047, as said below
- loader_shard: int32 [8192, 1], P(('groups', 'docs')), parts along dimension 0, may hold values from 0 to 15, as said below
Outputs:
- loaded_images: bfloat16 [16384, 1280], P(('groups', 'docs')), parts along dimension 0
- loaded_text: bfloat16 [16384, 1280], P(('groups', 'docs')), parts along dimension 0
The draws below stay inside these ranges and needn't reach their ends.
There are 2 independent parts, one for each index of `groups`. The reference program is written for one: setup_inputs(seed, part) draws one part's arguments, and reference() takes and returns one part's arrays. A program takes and returns all parts, laid end to end along the dimension named above; each array names one. Nothing has to cross between parts.
Inputs may be any that keep to these rules, and one draw needn't show every extreme that they name: `sent_doc`: documents are runs of 1 to 32 consecutive sentences, ids never falling. `image_owner`: the 256 images of one device name one owner at most 32 times, and some owner exactly 32 times. loader_shard = (a[source device] + b[image_owner]) mod 16 for two permutations a and b of the devices, drawn with the data. So the images of one device name one shard at most 32 times (some exactly 32), and the images that one owner receives from all devices name one shard at most 32 times, all from one source device. `anchor`: the image's document is the document of this sentence of its owner.
All inputs are finite; a program needn't handle non-finite values.
Results may differ from the reference program's by a relative error of at most 0.0048.
Values may be sent and summed in bfloat16 or wider, within the bound.
A program may use at most 64 MiB of HBM per device.

```python
import math
import jax
import jax.numpy as jnp
import numpy as np
from jax import lax

E = 1280
S_DEV = 2048
I_DEV = 256
MOST_SENT = 32
CAP = 32
SENTS = 32768
IMAGES = 4096
DOCS = 2048
SLOTS = 8192
N_DOCS = 16


def draw_sentences(key, part):
    base = jnp.clip(jax.random.normal(jax.random.fold_in(key, 11), (SENTS, E), jnp.float32), -6.0, 6.0)
    return base.astype(jnp.bfloat16)


def draw_images(key, part):
    base = jnp.clip(jax.random.normal(jax.random.fold_in(key, 13), (IMAGES, E), jnp.float32), -6.0, 6.0)
    return base.astype(jnp.bfloat16)


def draw_anchor(key, part):
    chooser = jax.random.randint(jax.random.fold_in(key, 21), (IMAGES,), 0, 4)
    nearby = jax.random.randint(jax.random.fold_in(key, 23), (IMAGES,), 0, 2 * MOST_SENT)
    edges = jnp.where(nearby < MOST_SENT, nearby, S_DEV - 2 * MOST_SENT + nearby)
    spread = jax.random.randint(jax.random.fold_in(key, 29), (IMAGES,), 0, S_DEV)
    return jnp.where(chooser == 0, edges, spread).astype(jnp.int32)


def route_pair(key):
    base = jax.random.fold_in(key, 31)
    listing = jnp.repeat(jnp.arange(N_DOCS, dtype=jnp.int32), CAP)
    total = N_DOCS * CAP
    leaning = jax.random.randint(jax.random.fold_in(base, 1), (N_DOCS,), 0, 3)
    chosen = jax.random.randint(jax.random.fold_in(base, 2), (N_DOCS,), 0, N_DOCS)
    noise = jax.random.randint(jax.random.fold_in(base, 3), (N_DOCS, total), 0, 4096)
    score = noise + leaning[listing][None, :] * 4096 + 1
    score = jnp.where(listing[None, :] == chosen[:, None], 0, score)
    score = score * total + jnp.arange(total, dtype=jnp.int32)[None, :]
    order = jnp.argsort(score, axis=1)
    owners = listing[order[:, :I_DEV]]
    spot_score = jax.random.randint(jax.random.fold_in(base, 4), (N_DOCS, I_DEV), 0, 4096) * I_DEV + jnp.arange(I_DEV, dtype=jnp.int32)[None, :]
    owners = jnp.take_along_axis(owners, jnp.argsort(spot_score, axis=1), axis=1)
    first_perm = jax.random.permutation(jax.random.fold_in(base, 5), N_DOCS).astype(jnp.int32)
    second_perm = jax.random.permutation(jax.random.fold_in(base, 6), N_DOCS).astype(jnp.int32)
    shards = (first_perm[:, None] + second_perm[owners]) % N_DOCS
    return (owners.reshape(IMAGES, 1).astype(jnp.int32), shards.reshape(IMAGES, 1).astype(jnp.int32))


def draw_image_owner(key, part):
    return route_pair(key)[0]


def draw_loader_shard(key, part):
    return route_pair(key)[1]


def profile(count, total, limit, skew):
    portions = [(1 << 20) // math.isqrt(rank ** skew) + 1 for rank in range(2, count + 1)]
    spare, holding = total - limit - (count - 1), [1] * (count - 1)
    while spare > 0:
        candidates = [i for i in range(count - 1) if holding[i] < limit]
        mass, budget = sum([portions[i] for i in candidates]), spare
        for i in candidates:
            more = min(limit - holding[i], max(1, budget * portions[i] // mass), spare)
            holding[i] = holding[i] + more
            spare = spare - more
    return np.array([limit] + holding)


def ragged(key, number_of, total, most, lean):
    if number_of == 2:
        one = jax.random.randint(key, (), max(1, total - most), min(most, total - 1) + 1)
        return jnp.stack([one, total - one])
    sizes = jnp.asarray(profile(number_of, total, most, lean), jnp.int32)
    pairs = (number_of - 1) // 2
    donor, receiver = sizes[1:1 + 2 * pairs:2], sizes[2:2 + 2 * pairs:2]
    room = jnp.minimum(donor - 1, most - receiver)
    shifted = jax.random.randint(jax.random.fold_in(key, 1), (pairs,), 0, 1 << 20) % (room + 1)
    sizes = sizes.at[1:1 + 2 * pairs:2].set(donor - shifted).at[2:2 + 2 * pairs:2].set(receiver + shifted)
    return sizes[jax.random.permutation(jax.random.fold_in(key, 2), number_of)]


def setup_inputs(seed: int = 0, part: int = 0) -> dict:
    streams_of = jax.random.split(jax.random.key(seed), 7)
    part_splits = jax.random.split(jax.random.fold_in(streams_of[6], part), 7)
    return {
        "sentences": draw_sentences(jax.random.fold_in(jax.random.fold_in(streams_of[6], part), 71), part),
        "sent_doc": jnp.searchsorted(jnp.cumsum(ragged(part_splits[1], DOCS, SENTS, MOST_SENT, 1)), jnp.arange(SENTS), side="right").astype(jnp.int32),
        "images": draw_images(jax.random.fold_in(jax.random.fold_in(streams_of[6], part), 71), part),
        "image_owner": draw_image_owner(jax.random.fold_in(jax.random.fold_in(streams_of[6], part), 71), part),
        "anchor": draw_anchor(jax.random.fold_in(jax.random.fold_in(streams_of[6], part), 71), part),
        "loader_shard": draw_loader_shard(jax.random.fold_in(jax.random.fold_in(streams_of[6], part), 71), part),
    }


def reference(sentences, sent_doc, images, image_owner, anchor, loader_shard):
    temper = E ** -0.5
    reach = MOST_SENT
    padded = jnp.pad(sentences, ((reach, reach), (0, 0)))
    padded_ids = jnp.pad(sent_doc, (reach, reach), constant_values=-1)
    centre = (image_owner[:, 0] * S_DEV + anchor).astype(jnp.int32)
    doc_ids = sent_doc[centre]
    offsets = jnp.arange(2 * reach + 1, dtype=jnp.int32)

    def align_block(pieces):
        queries, middle, owned = pieces
        indices = middle[:, None] + offsets[None, :]
        window = padded[indices].astype(jnp.float32)
        window_ids = padded_ids[indices]
        scores = jnp.einsum("be,bwe->bw", queries.astype(jnp.float32), window) * temper
        member = window_ids == owned[:, None]
        peak = jnp.max(jnp.where(member, scores, -1e30), axis=1, keepdims=True)
        raised = jnp.where(member, jnp.exp(scores - peak), 0.0)
        denominator = jnp.sum(raised, axis=1, keepdims=True)
        weights = (raised / denominator).astype(jnp.bfloat16)
        return jnp.einsum("bw,bwe->be", weights.astype(jnp.float32), window).astype(jnp.bfloat16)

    aligned = lax.map(align_block, (images.reshape(N_DOCS, I_DEV, E), centre.reshape(N_DOCS, I_DEV), doc_ids.reshape(N_DOCS, I_DEV)))
    aligned = aligned.reshape(IMAGES, E)
    targets = loader_shard[:, 0]
    sources = jnp.arange(IMAGES, dtype=jnp.int32) // I_DEV
    labels = jnp.arange(N_DOCS, dtype=jnp.int32)
    onehot = (targets[:, None] == labels[None, :]).astype(jnp.int32).reshape(N_DOCS, I_DEV, N_DOCS)
    ranking = jnp.sum((jnp.cumsum(onehot, axis=1) - 1) * onehot, axis=2).reshape(IMAGES)
    places = (targets * (N_DOCS * CAP) + sources * CAP + ranking).astype(jnp.int32)
    loaded_images = jnp.zeros((SLOTS, E), jnp.bfloat16).at[places].set(images)
    loaded_text = jnp.zeros((SLOTS, E), jnp.bfloat16).at[places].set(aligned)
    return loaded_images, loaded_text
```

```python
import functools

import jax
import jax.numpy as jnp
from jax import lax
from jax.experimental import pallas as pl
from jax.experimental.pallas import tpu as pltpu
from jax.sharding import PartitionSpec as P

MOST_SENT = 32
LANES = 128
SUB = 8
MESH = pl.DeviceIdType.MESH
HIGH = lax.Precision.HIGHEST
TRANS_LHS = (((0,), (0,)), ((), ()))
TRANS_RHS = (((1,), (1,)), ((), ()))


def iota(shape, dim):
    return lax.broadcasted_iota(jnp.int32, shape, dim)


def earlier(keys, n, above):
    onehot = (keys == iota((n, keys.shape[1]), 0)).astype(jnp.float32)
    counts = jnp.dot(onehot.astype(jnp.bfloat16), above, preferred_element_type=jnp.float32)
    return onehot, counts


def cuts(n, count, chunks):
    return [min(count, n * SUB * (q + 1)) for q in range(chunks - 1)] + [count]


def exchange_kernel(
    n, cap, chunks, owner_hbm, anchor_hbm, shard_hbm, images_hbm, ids_hbm, sent_hbm,
    img_out, txt_out,
    ext, owner_ref, anchor_ref, shard_ref, images_ref, own_ids, prev_ids, next_ids,
    ordered, keys_ref, far_images, far_keys, disp, shrd, far_disp, far_shrd,
    arrived, far_arrived, aligned, tsend, txt_in, meta_s, meta_in, target_ref,
    load_sem, local_sem, halo_send, halo_recv, raw_send, raw_recv, send_sem, recv_sem,
):
    me = lax.axis_index("docs")
    half = n // 2
    first = lax.div(me, half) * half
    across = lax.rem(first + half, n)
    partner = lax.rem(me + half, n)
    own_rows, feature = sent_hbm.shape
    width = ext.shape[0]
    count = images_hbm.shape[0]
    block = chunks * SUB
    group = half * SUB
    stripe = n * SUB
    part = half * block
    id_rows = own_rows // LANES
    temper = feature ** (-0.5)

    barrier = pltpu.get_barrier_semaphore()

    @pl.loop(1, n)
    def _(k):
        pl.semaphore_signal(barrier, inc=1, device_id={"docs": lax.rem(me + k, n)}, device_id_type=MESH)

    before = pl.multiple_of(jnp.maximum(me * id_rows - SUB, 0), SUB)
    after = pl.multiple_of(jnp.minimum(me * id_rows + id_rows, n * id_rows - SUB), SUB)
    loads = [
        pltpu.make_async_copy(src, dst, load_sem.at[i])
        for i, (src, dst) in enumerate((
            (owner_hbm, owner_ref),
            (anchor_hbm, anchor_ref),
            (shard_hbm, shard_ref),
            (images_hbm, images_ref),
            (ids_hbm.at[pl.ds(pl.multiple_of(me * id_rows, SUB), id_rows)], own_ids),
            (ids_hbm.at[pl.ds(before, SUB)], prev_ids),
            (ids_hbm.at[pl.ds(after, SUB)], next_ids),
            (sent_hbm, ext.at[pl.ds(0, own_rows)]),
        ))
    ]
    for copy in loads:
        copy.start()

    gap = LANES - 2 * MOST_SENT
    ext[pl.ds(own_rows + MOST_SENT, gap), :] = jnp.zeros((gap, feature), ext.dtype)
    above = (iota((count, count), 0) < iota((count, count), 1)).astype(jnp.bfloat16)
    for copy in loads[:3]:
        copy.wait()
    owner, anchor, shard = owner_ref[...], anchor_ref[...], shard_ref[...]
    onehot, counts = earlier(owner, n, above)
    rank = jnp.sum(counts * onehot, axis=0, keepdims=True).astype(jnp.int32)

    levels = -(-cap // SUB) * SUB
    onehot, counts = earlier(rank, levels, above)
    lower = (iota((levels, levels), 1) < iota((levels, levels), 0)).astype(jnp.bfloat16)
    under = jnp.dot(lower, onehot.astype(jnp.bfloat16), preferred_element_type=jnp.float32)
    under = jnp.sum(under, axis=1, keepdims=True)
    order = jnp.sum((counts + under) * onehot, axis=0, keepdims=True).astype(jnp.int32)
    sorter = (iota((count, count), 0) == order).astype(jnp.bfloat16)
    row = iota((SUB, count), 0)
    facts = jnp.where(row == 0, owner, jnp.where(row == 1, rank, shard))
    keys_ref[...] = lax.dot_general(
        facts.astype(jnp.bfloat16), sorter, TRANS_RHS, preferred_element_type=jnp.float32
    ).astype(jnp.int32)

    lane = iota((LANES, count), 0)
    lead = rank == 0
    for_owner = jnp.where(lane == rank, anchor + 1, 0) + jnp.where((lane == cap) & lead, shard + 1, 0)
    for_shard = jnp.where((lane == cap + 1) & lead, owner + 1, 0)
    keyed = lax.div(iota((stripe, count), 0), SUB)
    meta = lax.dot_general(
        (keyed == owner).astype(jnp.float32), for_owner.astype(jnp.float32), TRANS_RHS,
        precision=HIGH, preferred_element_type=jnp.float32,
    ) + lax.dot_general(
        (keyed == shard).astype(jnp.float32), for_shard.astype(jnp.float32), TRANS_RHS,
        precision=HIGH, preferred_element_type=jnp.float32,
    )
    meta_s[...] = meta.astype(jnp.int32)
    loads[3].wait()

    def pick(ref, start, size, place, values):
        tile = min(256, size)

        @pl.loop(0, size // tile)
        def _(t):
            base = pl.multiple_of(t * tile, tile)
            table = (place == iota((tile, place.shape[1]), 0) + base).astype(jnp.bfloat16)
            ref[pl.ds(start + base, tile), :] = jnp.dot(
                table, values, preferred_element_type=jnp.float32
            ).astype(jnp.bfloat16)

    def to_owner(who, order, q):
        inside = (who >= first) & (who < first + half)
        spot = (who - first) * SUB + lax.rem(order, SUB)
        if q is None:
            return jnp.where(inside, lax.div(order, SUB) * group + spot, -1)
        return jnp.where(inside & (lax.div(order, SUB) == q), spot, -1)

    pick(ordered, 0, count, order, images_ref[...])
    pick(disp, 0, part, to_owner(owner, rank, None), images_ref[...])
    pick(shrd, 0, part, (shard - first) * block + rank, images_ref[...])

    edges = cuts(n, count, chunks)
    ends = sorted(set(edges))

    def raw(piece):
        if piece < len(ends):
            low = ends[piece - 1] if piece else 0
            rows = pl.ds(low, ends[piece] - low)
            src, dst = ordered.at[rows], far_images.at[rows]
        else:
            src, dst = keys_ref, far_keys
        return pltpu.make_async_remote_copy(
            src_ref=src, dst_ref=dst, send_sem=raw_send.at[piece], recv_sem=raw_recv.at[piece],
            device_id={"docs": partner}, device_id_type=MESH,
        )

    def halo(way):
        to = lax.rem(me + 1, n) if way == 0 else lax.rem(me + n - 1, n)
        src = own_rows - MOST_SENT if way == 0 else 0
        dst = own_rows + LANES - MOST_SENT if way == 0 else own_rows
        return pltpu.make_async_remote_copy(
            src_ref=sent_hbm.at[pl.ds(src, MOST_SENT)], dst_ref=ext.at[pl.ds(dst, MOST_SENT)],
            send_sem=halo_send.at[way], recv_sem=halo_recv.at[way],
            device_id={"docs": to}, device_id_type=MESH,
        )

    META, SHRD, FSHRD, DISP = 0, 1, 2, 3
    FDISP, TEXT = DISP + chunks, DISP + 2 * chunks

    def route_of(kind, peer, sender):
        if kind == META:
            return meta_s, peer * SUB, meta_in, sender * SUB, SUB
        if kind == SHRD:
            return shrd, (peer - first) * block, img_out, sender * block, block
        if kind == FSHRD:
            return far_shrd, (peer - first) * block, img_out, lax.rem(sender + half, n) * block, block
        if kind < FDISP:
            base = (kind - DISP) * group
            return disp, base + (peer - first) * SUB, arrived, base + (sender - first) * SUB, SUB
        if kind < TEXT:
            base = (kind - FDISP) * group
            return far_disp, base + (peer - first) * SUB, far_arrived, base + (sender - first) * SUB, SUB
        base = (kind - TEXT) * stripe
        return tsend, base + peer * SUB, txt_in, base + sender * SUB, SUB

    def views(kind, peer, sender):
        src, src_at, dst, dst_at, size = route_of(kind, peer, sender)
        return (
            src.at[pl.ds(pl.multiple_of(src_at, size), size)],
            dst.at[pl.ds(pl.multiple_of(dst_at, size), size)],
        )

    def remote(kind, peer, sender):
        src, dst = views(kind, peer, sender)
        return pltpu.make_async_remote_copy(
            src_ref=src, dst_ref=dst,
            send_sem=send_sem.at[kind, peer], recv_sem=recv_sem.at[kind, sender],
            device_id={"docs": peer}, device_id_type=MESH,
        )

    def local(kind):
        src, dst = views(kind, me, me)
        return pltpu.make_async_copy(src, dst, local_sem.at[kind])

    def each(kind, act):
        if kind == META or kind >= TEXT:

            @pl.loop(0, half)
            def _(k):
                act(across + lax.rem(me - first + k, half))

        @pl.loop(1, half)
        def _(k):
            act(first + lax.rem(me - first + k, half))

    def start(kind):
        each(kind, lambda peer: remote(kind, peer, me).start())
        local(kind).start()

    def sent(kind):
        each(kind, lambda peer: remote(kind, peer, me).wait_send())

    def landed(kind):
        each(kind, lambda peer: remote(kind, peer, peer).wait_recv())
        local(kind).wait()

    pl.semaphore_wait(barrier, n - 1)
    start(META)
    halo(0).start()
    halo(1).start()
    raw(len(ends)).start()
    for q in range(chunks):
        start(DISP + q)
    start(SHRD)
    for piece in range(len(ends)):
        raw(piece).start()

    for copy in loads[4:]:
        copy.wait()
    for way in (0, 1):
        halo(way).wait_recv()
    landed(META)
    line = iota((1, LANES), 1)
    tail = jnp.where((line < MOST_SENT) & (me < n - 1), next_ids[0:1, :], -1)
    tail = jnp.where((line >= LANES - MOST_SENT) & (me > 0), prev_ids[SUB - 1 : SUB, :], tail)
    ids = jnp.concatenate([own_ids[r : r + 1, :] for r in range(id_rows)] + [tail], axis=1)

    def align(rows_ref, base, size, head):
        begin = pl.multiple_of(head * SUB, SUB)
        if size >= group:
            picked = jnp.concatenate([meta_in[pl.ds(begin, group), :]] * (size // group), axis=0)
        else:
            picked = meta_in[pl.ds(begin + base % group, size), :]
        spot = iota((size, 1), 0) + base
        inner = lax.rem(spot, SUB)
        step = lax.div(spot, group) * SUB + inner
        lanes = iota((size, LANES), 1)
        anchored = jnp.sum(jnp.where((lanes == step) & (lanes < cap), picked, 0), axis=1, keepdims=True)
        goal = jnp.sum(jnp.where(lanes == cap, picked, 0), axis=1, keepdims=True)
        target = (goal - 1) * SUB + inner
        filled = anchored > 0
        here = iota((size, width), 1) == anchored - 1
        doc = jnp.sum(jnp.where(here, ids, 0), axis=1, keepdims=True)
        doc = jnp.where(filled, doc, -2)
        scores = lax.dot_general(
            rows_ref[pl.ds(base, size), :], ext[...], TRANS_RHS, preferred_element_type=jnp.float32
        ) * temper
        member = doc == ids
        peak = jnp.max(jnp.where(member, scores, -1e30), axis=1, keepdims=True)
        raised = jnp.where(member, jnp.exp(scores - peak), 0.0)
        total = jnp.sum(raised, axis=1, keepdims=True)
        weights = (raised / jnp.where(filled, total, 1.0)).astype(jnp.bfloat16)
        result = jnp.dot(weights, ext[...], preferred_element_type=jnp.float32).astype(jnp.bfloat16)
        extra = 0 if rows_ref is arrived else group
        for low in range(0, size, group):
            at = (base + low) // group * stripe + (base + low) % group + extra
            high = min(size, low + group)
            aligned[pl.ds(at, high - low), :] = result[low:high]
            target_ref[pl.ds(at, high - low), :] = target[low:high]

    def align_all(rows_ref, base, rows, head):
        tile = min(256, rows)
        for low in range(base, base + rows, tile):
            align(rows_ref, low, tile, head)

    def route(q):
        begin = q * stripe
        tile = min(256, stripe)
        for base in range(0, stripe, tile):
            table = target_ref[pl.ds(begin, stripe), :] == iota((stripe, tile), 1) + base
            tsend[pl.ds(begin + base, tile), :] = lax.dot_general(
                table.astype(jnp.bfloat16), aligned[pl.ds(begin, stripe), :], TRANS_LHS,
                preferred_element_type=jnp.float32,
            ).astype(jnp.bfloat16)

    def place(q):
        wanted = jnp.sum(
            jnp.where(iota((stripe, LANES), 1) == cap + 1, meta_in[...], 0), axis=1, keepdims=True
        )
        wanted = (wanted - 1) * SUB + lax.rem(iota((stripe, 1), 0), SUB)
        tile = min(256, stripe)
        for base in range(0, stripe, tile):
            table = wanted[base : base + tile] == iota((tile, stripe), 1)
            moved = jnp.dot(
                table.astype(jnp.bfloat16), txt_in[pl.ds(q * stripe, stripe), :],
                preferred_element_type=jnp.float32,
            ).astype(jnp.bfloat16)
            for low in range(0, tile, SUB):
                at = (base + low) // SUB * block + q * SUB
                txt_out[pl.ds(at, SUB), :] = moved[low : low + SUB]

    for q in range(chunks):
        landed(DISP + q)
    align_all(arrived, 0, part, first)

    raw(len(ends)).wait_recv()
    far_owner, far_rank, far_shard = far_keys[0:1, :], far_keys[1:2, :], far_keys[2:3, :]

    def far_fill(q):
        rows = edges[q]
        place_of = to_owner(far_owner, far_rank, q)[:, :rows]
        pick(far_disp, q * group, group, place_of, far_images[pl.ds(0, rows), :])
        start(FDISP + q)

    ready = []
    for piece, end in enumerate(ends):
        last = piece == len(ends) - 1
        raw(piece).wait_recv()
        due = [q for q in range(chunks) if edges[q] == end]
        for i, q in enumerate(due):
            far_fill(q)
            if last and i == 0:
                for old in ready:
                    start(TEXT + old)
        if last:
            pick(far_shrd, 0, part, (far_shard - first) * block + far_rank, far_images[...])
            start(FSHRD)
        for q in due:
            landed(FDISP + q)
            align_all(far_arrived, q * group, group, across)
            route(q)
            if last:
                start(TEXT + q)
            else:
                ready.append(q)

    landed(SHRD)
    landed(FSHRD)
    for q in range(chunks):
        landed(TEXT + q)
        place(q)
    for way in (0, 1):
        halo(way).wait_send()
    for piece in range(len(ends) + 1):
        raw(piece).wait_send()
    for kind in range(TEXT + chunks):
        sent(kind)


def store_kernel(img_ref, txt_ref, img_out, txt_out, sems):
    copies = [
        pltpu.make_async_copy(src, dst, sems.at[i])
        for i, (src, dst) in enumerate(((img_ref, img_out), (txt_ref, txt_out)))
    ]
    for copy in copies:
        copy.start()
    for copy in copies:
        copy.wait()


def shards(sentences, sent_doc, images, image_owner, anchor, loader_shard):
    n = lax.axis_size("docs")
    own_rows, feature = sentences.shape
    count = images.shape[0]
    cap = max(4, 2 * count // n)
    chunks = -(-cap // SUB)
    block = chunks * SUB
    rows = n * block
    width = own_rows + LANES
    pieces = len(set(cuts(n, count, chunks)))
    kinds = 3 + 3 * chunks
    slots = pltpu.VMEM((rows, feature), jnp.bfloat16)
    some = pltpu.VMEM((rows // 2, feature), jnp.bfloat16)
    held = pltpu.VMEM((count, feature), jnp.bfloat16)
    vector = pltpu.VMEM((1, count), jnp.int32)
    table = pltpu.VMEM((n * SUB, LANES), jnp.int32)
    anywhere = pl.BlockSpec(memory_space=pl.ANY)
    dma = pltpu.SemaphoreType.DMA
    vmem = pl.BlockSpec(memory_space=pltpu.VMEM)
    image, text = pl.pallas_call(
        functools.partial(exchange_kernel, n, cap, chunks),
        out_shape=(slots, slots),
        in_specs=[anywhere] * 6,
        out_specs=(vmem, vmem),
        scratch_shapes=[
            pltpu.VMEM((width, feature), jnp.bfloat16),
            vector, vector, vector, held,
            pltpu.VMEM((own_rows // LANES, LANES), jnp.int32),
            pltpu.VMEM((SUB, LANES), jnp.int32),
            pltpu.VMEM((SUB, LANES), jnp.int32),
            held, pltpu.VMEM((SUB, count), jnp.int32),
            held, pltpu.VMEM((SUB, count), jnp.int32),
            some, some, some, some, some, some, slots, slots, slots, table, table,
            pltpu.VMEM((rows, 1), jnp.int32),
            dma((8,)), dma((kinds,)), dma((2,)), dma((2,)), dma((pieces + 1,)), dma((pieces + 1,)),
            dma((kinds, n)), dma((kinds, n)),
        ],
        compiler_params=pltpu.CompilerParams(
            collective_id=0, has_side_effects=True, vmem_limit_bytes=48 * 1024 * 1024
        ),
    )(image_owner.T, anchor[None, :], loader_shard.T, images, sent_doc.reshape(-1, LANES), sentences)
    if block != cap:
        return tuple(
            array.reshape(n, block, feature)[:, :cap].reshape(n * cap, feature) for array in (image, text)
        )
    image, text = (pltpu.with_memory_space_constraint(array, pltpu.VMEM) for array in (image, text))
    full = jax.ShapeDtypeStruct((rows, feature), jnp.bfloat16)
    return pl.pallas_call(
        store_kernel,
        out_shape=(full, full),
        in_specs=[vmem, vmem],
        out_specs=(anywhere, anywhere),
        scratch_shapes=[dma((2,))],
    )(image, text)


def solution(mesh):
    return jax.shard_map(
        shards,
        mesh=mesh,
        in_specs=(
            P(("groups", "docs"), None),
            P("groups"),
            P(("groups", "docs"), None),
            P(("groups", "docs"), None),
            P(("groups", "docs")),
            P(("groups", "docs"), None),
        ),
        out_specs=(P(("groups", "docs"), None), P(("groups", "docs"), None)),
        check_vma=False,
    )
```

```python
import functools

import jax
import jax.numpy as jnp
from jax import lax
from jax.experimental import pallas as pl
from jax.experimental.pallas import tpu as pltpu
from jax.sharding import PartitionSpec as P

MOST_SENT = 32
LANES = 128
SUB = 8
MESH = pl.DeviceIdType.MESH
HIGH = lax.Precision.HIGHEST
TRANS_LHS = (((0,), (0,)), ((), ()))
TRANS_RHS = (((1,), (1,)), ((), ()))


def iota(shape, dim):
    return lax.broadcasted_iota(jnp.int32, shape, dim)


def earlier(keys, n, above):
    onehot = (keys == iota((n, keys.shape[1]), 0)).astype(jnp.float32)
    counts = jnp.dot(onehot.astype(jnp.bfloat16), above, preferred_element_type=jnp.float32)
    return onehot, counts


def segments(n, count):
    first = min(count, n * SUB)
    middle = (first + count) // 2 // SUB * SUB
    return [(0, first)] + [piece for piece in ((first, middle), (middle, count)) if piece[0] < piece[1]]


def exchange_kernel(
    n, cap, chunks, owner_hbm, anchor_hbm, shard_hbm, images_hbm, ids_hbm, sent_hbm,
    img_out, txt_out,
    ext, owner_ref, anchor_ref, shard_ref, images_ref, own_ids, prev_ids, next_ids,
    ordered, keys_ref, far_images, far_keys, disp, shrd, far_disp, far_shrd,
    arrived, far_arrived, aligned, tsend, txt_in, meta_s, meta_in, target_ref,
    load_sem, halo_send, halo_recv, raw_send, raw_recv, send_sem, recv_sem,
):
    me = lax.axis_index("docs")
    half = n // 2
    first = lax.div(me, half) * half
    across = lax.rem(first + half, n)
    partner = lax.rem(me + half, n)
    own_rows, feature = sent_hbm.shape
    width = ext.shape[0]
    count = images_hbm.shape[0]
    block = chunks * SUB
    group = half * SUB
    stripe = n * SUB
    part = half * block
    id_rows = own_rows // LANES
    temper = feature ** (-0.5)

    ext[pl.ds(own_rows, LANES), :] = jnp.zeros((LANES, feature), ext.dtype)
    barrier = pltpu.get_barrier_semaphore()

    @pl.loop(1, n)
    def _(k):
        pl.semaphore_signal(barrier, inc=1, device_id={"docs": lax.rem(me + k, n)}, device_id_type=MESH)

    before = pl.multiple_of(jnp.maximum(me * id_rows - SUB, 0), SUB)
    after = pl.multiple_of(jnp.minimum(me * id_rows + id_rows, n * id_rows - SUB), SUB)
    loads = [
        pltpu.make_async_copy(src, dst, load_sem.at[i])
        for i, (src, dst) in enumerate((
            (owner_hbm, owner_ref),
            (anchor_hbm, anchor_ref),
            (shard_hbm, shard_ref),
            (images_hbm, images_ref),
            (ids_hbm.at[pl.ds(pl.multiple_of(me * id_rows, SUB), id_rows)], own_ids),
            (ids_hbm.at[pl.ds(before, SUB)], prev_ids),
            (ids_hbm.at[pl.ds(after, SUB)], next_ids),
            (sent_hbm, ext.at[pl.ds(0, own_rows)]),
        ))
    ]
    for copy in loads:
        copy.start()

    above = (iota((count, count), 0) < iota((count, count), 1)).astype(jnp.bfloat16)
    for copy in loads[:3]:
        copy.wait()
    owner, anchor, shard = owner_ref[...], anchor_ref[...], shard_ref[...]
    onehot, counts = earlier(owner, n, above)
    rank = jnp.sum(counts * onehot, axis=0, keepdims=True).astype(jnp.int32)

    def pick(ref, start, size, place, values):
        tile = min(256, size)

        @pl.loop(0, size // tile)
        def _(t):
            base = pl.multiple_of(t * tile, tile)
            table = (place == iota((tile, place.shape[1]), 0) + base).astype(jnp.bfloat16)
            ref[pl.ds(start + base, tile), :] = jnp.dot(
                table, values, preferred_element_type=jnp.float32
            ).astype(jnp.bfloat16)

    def to_owner(who, order, q):
        inside = (who >= first) & (who < first + half)
        spot = (who - first) * SUB + lax.rem(order, SUB)
        if q is None:
            return jnp.where(inside, lax.div(order, SUB) * group + spot, -1)
        return jnp.where(inside & (lax.div(order, SUB) == q), spot, -1)

    pieces = segments(n, count)
    keys = len(pieces)

    def raw(piece):
        if piece < keys:
            rows = pl.ds(pieces[piece][0], pieces[piece][1] - pieces[piece][0])
            src, dst = ordered.at[rows], far_images.at[rows]
        else:
            src, dst = keys_ref, far_keys
        return pltpu.make_async_remote_copy(
            src_ref=src, dst_ref=dst, send_sem=raw_send.at[piece], recv_sem=raw_recv.at[piece],
            device_id={"docs": partner}, device_id_type=MESH,
        )

    def halo(way):
        to = me + 1 if way == 0 else me - 1
        src = own_rows - MOST_SENT if way == 0 else 0
        dst = own_rows + LANES - MOST_SENT if way == 0 else own_rows
        return pltpu.make_async_remote_copy(
            src_ref=sent_hbm.at[pl.ds(src, MOST_SENT)], dst_ref=ext.at[pl.ds(dst, MOST_SENT)],
            send_sem=halo_send.at[way], recv_sem=halo_recv.at[way],
            device_id={"docs": to}, device_id_type=MESH,
        )

    def halos(act):
        @pl.when(me < n - 1)
        def _():
            act(0, 1)

        @pl.when(me > 0)
        def _():
            act(1, 0)

    open_sends, open_landings = [], []

    META, DISP, SHRD, FSHRD, FDISP = 0, 1, 2, 3, 4
    TEXT = FDISP + chunks

    def ends(kind):
        if kind == META:
            return meta_s, meta_in, 1, 1
        if kind == DISP:
            return disp, arrived, SUB, chunks
        if kind == SHRD:
            return shrd, img_out, block, 1
        if kind == FSHRD:
            return far_shrd, img_out, block, 1
        if kind < TEXT:
            return far_disp, far_arrived, SUB, 1
        return tsend, txt_in, SUB, 1

    def views(kind, peer, q):
        src, dst, rows, _ = ends(kind)
        to, slot = peer - first, me - first
        src_at, dst_at = to * SUB, slot * SUB
        if kind == META:
            src_at, dst_at = peer * SUB, me * SUB
        elif kind == DISP:
            src_at, dst_at = src_at + q * group, dst_at + q * group
        elif kind == SHRD:
            src_at, dst_at = to * block, me * block
        elif kind == FSHRD:
            src_at, dst_at = to * block, partner * block
        elif kind < TEXT:
            base = (kind - FDISP) * group
            src_at, dst_at = base + src_at, base + dst_at
        else:
            base = (kind - TEXT) * stripe
            src_at, dst_at = base + peer * SUB, base + me * SUB
        return (
            src.at[pl.ds(pl.multiple_of(src_at, SUB), rows)],
            dst.at[pl.ds(pl.multiple_of(dst_at, SUB), rows)],
        )

    def everyone(kind):
        return kind == META or kind >= TEXT

    def each(kind, act):
        for q in range(ends(kind)[3]):
            if everyone(kind):

                @pl.loop(0, half)
                def _(k):
                    act(across + lax.rem(me - first + k, half), q)

            @pl.loop(1, half)
            def _(k):
                act(first + lax.rem(me - first + k, half), q)

    def send(kind, peer, q):
        src, dst = views(kind, peer, q)
        pltpu.make_async_remote_copy(
            src_ref=src, dst_ref=dst, send_sem=send_sem.at[kind], recv_sem=recv_sem.at[kind],
            device_id={"docs": peer}, device_id_type=MESH,
        ).start()

    def whole(kind, less):
        src, dst, rows, times = ends(kind)
        rows = pl.ds(0, rows * times * ((n if everyone(kind) else half) - less))
        return pltpu.make_async_remote_copy(
            src_ref=src.at[rows], dst_ref=dst.at[rows], send_sem=send_sem.at[kind],
            recv_sem=recv_sem.at[kind], device_id={"docs": partner}, device_id_type=MESH,
        )

    def start(kind):
        open_sends.append(kind)
        open_landings.append(kind)
        each(kind, functools.partial(send, kind))
        for q in range(ends(kind)[3]):
            src, dst = views(kind, me, q)
            pltpu.make_async_copy(src, dst, recv_sem.at[kind]).start()

    def start_raw(piece):
        open_sends.append(-1 - piece)
        open_landings.append(-1 - piece)
        raw(piece).start()

    def landed_raw(piece):
        open_landings.remove(-1 - piece)
        raw(piece).wait_recv()

    def sent(kind):
        whole(kind, 1).wait_send()

    def landed(kind):
        open_landings.remove(kind)
        whole(kind, 0).wait_recv()

    def finish():
        for kind in list(open_landings):
            landed_raw(-1 - kind) if kind < 0 else landed(kind)
        for kind in open_sends:
            raw(-1 - kind).wait_send() if kind < 0 else sent(kind)
        halos(lambda out, back: halo(out).wait_send())

    lane = iota((LANES, count), 0)
    lead = rank == 0
    for_owner = jnp.where(lane == rank, anchor + 1, 0) + jnp.where((lane == cap) & lead, shard + 1, 0)
    for_shard = jnp.where((lane == cap + 1) & lead, owner + 1, 0)
    keyed = lax.div(iota((stripe, count), 0), SUB)
    meta = lax.dot_general(
        (keyed == owner).astype(jnp.float32), for_owner.astype(jnp.float32), TRANS_RHS,
        precision=HIGH, preferred_element_type=jnp.float32,
    ) + lax.dot_general(
        (keyed == shard).astype(jnp.float32), for_shard.astype(jnp.float32), TRANS_RHS,
        precision=HIGH, preferred_element_type=jnp.float32,
    )
    meta_s[...] = meta.astype(jnp.int32)
    levels = -(-cap // SUB) * SUB
    onehot, counts = earlier(rank, levels, above)
    lower = (iota((levels, levels), 1) < iota((levels, levels), 0)).astype(jnp.bfloat16)
    under = jnp.dot(lower, onehot.astype(jnp.bfloat16), preferred_element_type=jnp.float32)
    under = jnp.sum(under, axis=1, keepdims=True)
    order = jnp.sum((counts + under) * onehot, axis=0, keepdims=True).astype(jnp.int32)
    sorter = (iota((count, count), 0) == order).astype(jnp.bfloat16)
    row = iota((SUB, count), 0)
    facts = jnp.where(row == 0, owner, jnp.where(row == 1, rank, shard))
    keys_ref[...] = lax.dot_general(
        facts.astype(jnp.bfloat16), sorter, TRANS_RHS, preferred_element_type=jnp.float32
    ).astype(jnp.int32)
    loads[3].wait()
    pick(disp, 0, part, to_owner(owner, rank, None), images_ref[...])
    pick(ordered, 0, count, order, images_ref[...])
    pl.semaphore_wait(barrier, n - 1)
    start(DISP)
    start(META)
    halos(lambda out, back: halo(out).start())
    start_raw(keys)
    for piece in range(keys):
        start_raw(piece)
    pick(shrd, 0, part, (shard - first) * block + rank, images_ref[...])
    start(SHRD)
    for copy in loads[4:]:
        copy.wait()
    halos(lambda out, back: halo(back).wait_recv())
    landed(META)
    meta_all = jnp.broadcast_to(
        meta_in[...].reshape(n, SUB, LANES)[:, :1], (n, SUB, LANES)
    ).reshape(stripe, LANES)
    meta_in[...] = meta_all
    line = iota((1, LANES), 1)
    tail = jnp.where((line < MOST_SENT) & (me < n - 1), next_ids[0:1, :], -1)
    tail = jnp.where((line >= LANES - MOST_SENT) & (me > 0), prev_ids[SUB - 1 : SUB, :], tail)
    ids = jnp.concatenate([own_ids[r : r + 1, :] for r in range(id_rows)] + [tail], axis=1)

    def align(rows_ref, base, size, head):
        begin = pl.multiple_of(head * SUB, SUB)
        if size >= group:
            picked = jnp.concatenate([meta_in[pl.ds(begin, group), :]] * (size // group), axis=0)
        else:
            picked = meta_in[pl.ds(begin + base % group, size), :]
        spot = iota((size, 1), 0) + base
        inner = lax.rem(spot, SUB)
        step = lax.div(spot, group) * SUB + inner
        lanes = iota((size, LANES), 1)
        anchored = jnp.sum(jnp.where((lanes == step) & (lanes < cap), picked, 0), axis=1, keepdims=True)
        goal = jnp.sum(jnp.where(lanes == cap, picked, 0), axis=1, keepdims=True)
        target = (goal - 1) * SUB + inner
        filled = anchored > 0
        here = iota((size, width), 1) == anchored - 1
        doc = jnp.sum(jnp.where(here, ids, 0), axis=1, keepdims=True)
        doc = jnp.where(filled, doc, -2)
        scores = lax.dot_general(
            rows_ref[pl.ds(base, size), :], ext[...], TRANS_RHS, preferred_element_type=jnp.float32
        ) * temper
        member = doc == ids
        peak = jnp.max(jnp.where(member, scores, -1e30), axis=1, keepdims=True)
        raised = jnp.where(member, jnp.exp(scores - peak), 0.0)
        total = jnp.sum(raised, axis=1, keepdims=True)
        weights = (raised / jnp.where(filled, total, 1.0)).astype(jnp.bfloat16)
        result = jnp.dot(weights, ext[...], preferred_element_type=jnp.float32).astype(jnp.bfloat16)
        extra = 0 if rows_ref is arrived else group
        for low in range(0, size, group):
            at = (base + low) // group * stripe + (base + low) % group + extra
            high = min(size, low + group)
            aligned[pl.ds(at, high - low), :] = result[low:high]
            target_ref[pl.ds(at, high - low), :] = target[low:high]

    def align_all(rows_ref, base, rows, head):
        tile = min(256, rows)
        for low in range(base, base + rows, tile):
            align(rows_ref, low, tile, head)

    def route(q):
        begin = q * stripe
        tile = min(256, stripe)
        for base in range(0, stripe, tile):
            table = target_ref[pl.ds(begin, stripe), :] == iota((stripe, tile), 1) + base
            tsend[pl.ds(begin + base, tile), :] = lax.dot_general(
                table.astype(jnp.bfloat16), aligned[pl.ds(begin, stripe), :], TRANS_LHS,
                preferred_element_type=jnp.float32,
            ).astype(jnp.bfloat16)

    def place(q):
        wanted = jnp.sum(
            jnp.where(iota((stripe, LANES), 1) == cap + 1, meta_in[...], 0), axis=1, keepdims=True
        )
        wanted = (wanted - 1) * SUB + lax.rem(iota((stripe, 1), 0), SUB)
        tile = min(256, stripe)
        for base in range(0, stripe, tile):
            table = wanted[base : base + tile] == iota((tile, stripe), 1)
            moved = jnp.dot(
                table.astype(jnp.bfloat16), txt_in[pl.ds(q * stripe, stripe), :],
                preferred_element_type=jnp.float32,
            ).astype(jnp.bfloat16)
            for low in range(0, tile, SUB):
                at = (base + low) // SUB * block + q * SUB
                txt_out[pl.ds(at, SUB), :] = moved[low : low + SUB]

    landed(DISP)

    landed_raw(keys)
    far_owner, far_rank, far_shard = far_keys[0:1, :], far_keys[1:2, :], far_keys[2:3, :]

    def far_fill(q):
        rows = pieces[0][1] if q == 0 else count
        place_of = to_owner(far_owner, far_rank, q)[:, :rows]
        pick(far_disp, q * group, group, place_of, far_images[pl.ds(0, rows), :])
        start(FDISP + q)

    def far_align(q):
        landed(FDISP + q)
        align_all(far_arrived, q * group, group, across)
        route(q)

    landed_raw(0)
    far_fill(0)
    align_all(arrived, 0, part, first)
    for piece in range(1, keys):
        landed_raw(piece)
    for q in range(1, chunks):
        far_fill(q)
    pick(far_shrd, 0, part, (far_shard - first) * block + far_rank, far_images[...])
    start(FSHRD)
    far_align(0)
    start(TEXT)
    for q in range(1, chunks):
        far_align(q)
        start(TEXT + q)
    for q in range(chunks):
        landed(TEXT + q)
        place(q)
    finish()


def store_kernel(img_ref, txt_ref, img_out, txt_out, sems):
    copies = [
        pltpu.make_async_copy(src, dst, sems.at[i])
        for i, (src, dst) in enumerate(((img_ref, img_out), (txt_ref, txt_out)))
    ]
    for copy in copies:
        copy.start()
    for copy in copies:
        copy.wait()


def shards(sentences, sent_doc, images, image_owner, anchor, loader_shard):
    n = lax.axis_size("docs")
    own_rows, feature = sentences.shape
    count = images.shape[0]
    cap = max(4, 2 * count // n)
    chunks = -(-cap // SUB)
    block = chunks * SUB
    rows = n * block
    width = own_rows + LANES
    pieces = len(segments(n, count))
    kinds = 4 + 2 * chunks
    slots = pltpu.VMEM((rows, feature), jnp.bfloat16)
    some = pltpu.VMEM((rows // 2, feature), jnp.bfloat16)
    held = pltpu.VMEM((count, feature), jnp.bfloat16)
    vector = pltpu.VMEM((1, count), jnp.int32)
    table = pltpu.VMEM((n * SUB, LANES), jnp.int32)
    anywhere = pl.BlockSpec(memory_space=pl.ANY)
    dma = pltpu.SemaphoreType.DMA
    vmem = pl.BlockSpec(memory_space=pltpu.VMEM)
    image, text = pl.pallas_call(
        functools.partial(exchange_kernel, n, cap, chunks),
        out_shape=(slots, slots),
        in_specs=[anywhere] * 6,
        out_specs=(vmem, vmem),
        scratch_shapes=[
            pltpu.VMEM((width, feature), jnp.bfloat16),
            vector, vector, vector, held,
            pltpu.VMEM((own_rows // LANES, LANES), jnp.int32),
            pltpu.VMEM((SUB, LANES), jnp.int32),
            pltpu.VMEM((SUB, LANES), jnp.int32),
            held, pltpu.VMEM((SUB, count), jnp.int32),
            held, pltpu.VMEM((SUB, count), jnp.int32),
            some, some, some, some, some, some, slots, slots, slots, table, table,
            pltpu.VMEM((rows, 1), jnp.int32),
            dma((8,)), dma((2,)), dma((2,)), dma((pieces + 1,)), dma((pieces + 1,)),
            dma((kinds,)), dma((kinds,)),
        ],
        compiler_params=pltpu.CompilerParams(
            collective_id=0, has_side_effects=True, vmem_limit_bytes=min(60, 63 - 4 * rows * feature // 2**20) * 2**20
        ),
    )(image_owner.T, anchor[None, :], loader_shard.T, images, sent_doc.reshape(-1, LANES), sentences)
    if block != cap:
        return tuple(
            array.reshape(n, block, feature)[:, :cap].reshape(n * cap, feature) for array in (image, text)
        )
    image, text = (pltpu.with_memory_space_constraint(array, pltpu.VMEM) for array in (image, text))
    full = jax.ShapeDtypeStruct((rows, feature), jnp.bfloat16)
    return pl.pallas_call(
        store_kernel,
        out_shape=(full, full),
        in_specs=[vmem, vmem],
        out_specs=(anywhere, anywhere),
        scratch_shapes=[dma((2,))],
        compiler_params=pltpu.CompilerParams(vmem_limit_bytes=1024 * 1024),
    )(image, text)


def solution(mesh):
    return jax.shard_map(
        shards,
        mesh=mesh,
        in_specs=(
            P(("groups", "docs"), None),
            P("groups"),
            P(("groups", "docs"), None),
            P(("groups", "docs"), None),
            P(("groups", "docs")),
            P(("groups", "docs"), None),
        ),
        out_specs=(P(("groups", "docs"), None), P(("groups", "docs"), None)),
        check_vma=False,
    )
```
